32 devices in a mesh: rep: 4 (over x, y), dp: 8 (over z, core).
Axes of the slice: x: 2, y: 2, z: 4, core: 2. Of those that a mesh axis runs over, the one named last changes fastest.
Arguments:
- x: bfloat16 [32, 4096, 896], P(('rep', 'dp')), parts along dimension 0
- dy: bfloat16 [32, 4096, 896], P(('rep', 'dp')), parts along dimension 0
- w_gate: bfloat16 [2, 896, 2304], P(None, 'dp')
- w_up: bfloat16 [2, 896, 2304], P(None, 'dp')
- w_down: bfloat16 [2, 2304, 896], P(None, 'dp')
Outputs:
- output 1: bfloat16 [32, 4096, 896], P(('rep', 'dp')), parts along dimension 0
- output 2: bfloat16 [8, 896, 2304], P('rep', 'dp'), parts along dimension 0
- output 3: bfloat16 [8, 896, 2304], P('rep', 'dp'), parts along dimension 0
- output 4: bfloat16 [8, 2304, 896], P('rep', 'dp'), parts along dimension 0
There are 4 independent parts. The reference program is written for one: setup_inputs(seed, part) draws one part's arguments, and reference() takes and returns one part's arrays. A program takes and returns all parts, laid end to end along the dimension named above; an argument that names none is the same for every part.
All inputs are finite; a program needn't handle non-finite values.
Results may differ from the reference program's by a relative error of at most 0.018.
Values are sent between devices in bfloat16 or wider.
A program may use at most 2 GiB of HBM per device.

```python
import jax
import jax.numpy as jnp
from jax import lax

SEQUENCES = 8
TOKENS = 4096
D = 896
FF = 2304
LAYERS = 2
NAMES = ("w_gate", "w_up", "w_down")
SHAPES = {"w_gate": (LAYERS, D, FF), "w_up": (LAYERS, D, FF), "w_down": (LAYERS, FF, D)}


def bump(key, n, height):
    away = (jnp.arange(n, dtype=jnp.int32) - jax.random.randint(key, (), 0, n, jnp.int32)) % n
    return jnp.where(away < n // 8, height, 1.0)


def together(key, own, strength):
    shared = jax.random.normal(key, own.shape[1:], jnp.float32)
    return (own + strength * shared) * lax.rsqrt(1 + strength * strength)


def setup_inputs(seed: int = 0, part: int = 0) -> dict:
    kx, kdy, ka, kb, kz, kf, kh, kl, *kw = jax.random.split(jax.random.key(seed), 8 + len(NAMES))
    kx, kdy, ka, kb = (jax.random.fold_in(k, part) for k in (kx, kdy, ka, kb))
    shape = (SEQUENCES, TOKENS, D)
    much_x, much_dy = jax.random.uniform(kz, (2,), jnp.float32, 0.0, 1.0)
    layers = 2.0 ** jax.random.uniform(kl, (LAYERS, 1, 1), jnp.float32, -1.0, 1.0)
    x = together(ka, jax.random.normal(kx, shape, jnp.float32), much_x) * bump(kf, D, 4.0)
    dy = together(kb, jax.random.normal(kdy, shape, jnp.float32), much_dy)
    drawn = {"x": x.astype(jnp.bfloat16), "dy": (dy * (SEQUENCES * TOKENS) ** -0.5).astype(jnp.bfloat16)}
    for key, name in zip(kw, NAMES, strict=True):
        w = jax.random.normal(key, SHAPES[name], jnp.float32) * SHAPES[name][1] ** -0.5
        drawn[name] = (w * {"w_gate": 1.0, "w_up": bump(kh, FF, 4.0), "w_down": layers}[name]).astype(jnp.bfloat16)
    return drawn


def matmul(a, w):
    return jnp.dot(a, w, preferred_element_type=jnp.float32).astype(jnp.bfloat16)


def normed(h):
    wide = h.astype(jnp.float32)
    scale = lax.rsqrt(jnp.mean(wide**2, -1, keepdims=True) + 1e-6)
    return (wide * scale).astype(jnp.bfloat16)


def layer(h, w):
    a = normed(h)
    gate = jnp.dot(a, w["w_gate"], preferred_element_type=jnp.float32)
    up = jnp.dot(a, w["w_up"], preferred_element_type=jnp.float32)
    return h + matmul((jax.nn.silu(gate) * up).astype(jnp.bfloat16), w["w_down"])


def stack(weights, h):
    return lax.scan(lambda h, w: (layer(h, w), None), h, weights)[0]


def reference(x, dy, w_gate, w_up, w_down):
    weights = dict(zip(NAMES, (w_gate, w_up, w_down), strict=True))

    def take(so_far, sequence):
        h, by_y = sequence
        _, back = jax.vjp(stack, weights, h)
        by_weights, by_h = back(by_y)
        return jax.tree.map(lambda total, term: total + term.astype(jnp.float32), so_far, by_weights), by_h

    none_yet = {name: jnp.zeros(w.shape, jnp.float32) for name, w in weights.items()}
    by_weights, by_x = lax.scan(take, none_yet, (x, dy))
    return (by_x, *(by_weights[name].astype(jnp.bfloat16) for name in NAMES))
```

```python
import functools

import jax
import jax.numpy as jnp
from jax import lax
from jax.experimental import pallas as pl
from jax.experimental.pallas import tpu as pltpu
from jax.sharding import PartitionSpec as P

TOK, D, FF, L, DP = 4096, 896, 2304, 2, 8
CW = 256
NCH = FF // CW
KR = FF // DP // NCH
DR = D // DP
T = 1024
NT = TOK // T
SUB = 256
NP = L * NCH
EPS = 1e-6
MESH = pl.DeviceIdType.MESH
F32, BF16 = jnp.float32, jnp.bfloat16
VMEM_LIMIT = 60 * 1024 * 1024


def dot(a, b, ca, cb):
    return lax.dot_general(a, b, (((ca,), (cb,)), ((), ())), preferred_element_type=F32)


def sigmoid(g):
    return 0.5 * jnp.tanh(0.5 * g) + 0.5


def scale_of(h):
    return lax.rsqrt(jnp.mean(h * h, -1, keepdims=True) + EPS)


def forward_kernel(x_ref, wg_ref, wu_ref, wd_ref, g_ref, u_ref, h_ref, a_s, acc):
    c = pl.program_id(1)

    @pl.when(c == 0)
    def _():
        for i in range(T // SUB):
            rows = pl.ds(i * SUB, SUB)
            h = x_ref[rows, :].astype(F32)
            a_s[rows, :] = (h * scale_of(h)).astype(BF16)
        acc[...] = jnp.zeros_like(acc)

    wg = wg_ref[:, 0, c].reshape(D, CW)
    wu = wu_ref[:, 0, c].reshape(D, CW)
    wd = wd_ref[:, 0, c].reshape(CW, D)
    for i in range(T // SUB):
        rows = pl.ds(i * SUB, SUB)
        a = a_s[rows, :]
        g = dot(a, wg, 1, 0)
        u = dot(a, wu, 1, 0)
        g_ref[rows, :] = g
        u_ref[rows, :] = u
        p = (g * sigmoid(g) * u).astype(BF16)
        acc[rows, :] += dot(p, wd, 1, 0)

    @pl.when(c == NCH - 1)
    def _():
        h_ref[...] = x_ref[...] + acc[...].astype(BF16)


def forward(x, wg, wu, wd):
    whole = lambda *s: pl.BlockSpec(s, lambda t, c: (0, 0, 0, 0, 0))
    return pl.pallas_call(
        forward_kernel,
        grid=(NT, NCH),
        in_specs=[
            pl.BlockSpec((T, D), lambda t, c: (t, 0)),
            whole(DP, 1, NCH, DR, CW),
            whole(DP, 1, NCH, DR, CW),
            whole(DP, 1, NCH, KR, D),
        ],
        out_specs=[
            pl.BlockSpec((T, CW), lambda t, c: (t, c)),
            pl.BlockSpec((T, CW), lambda t, c: (t, c)),
            pl.BlockSpec((T, D), lambda t, c: (t, 0)),
        ],
        out_shape=[
            jax.ShapeDtypeStruct((TOK, FF), F32),
            jax.ShapeDtypeStruct((TOK, FF), F32),
            jax.ShapeDtypeStruct((TOK, D), BF16),
        ],
        scratch_shapes=[pltpu.VMEM((T, D), BF16), pltpu.VMEM((T, D), F32)],
        compiler_params=pltpu.CompilerParams(
            vmem_limit_bytes=VMEM_LIMIT, dimension_semantics=("arbitrary", "arbitrary")
        ),
        cost_estimate=pl.CostEstimate(flops=6 * TOK * D * FF, bytes_accessed=10**8, transcendentals=0),
        name="forward",
    )(x, wg, wu, wd)


def backward_kernel(
    x_ref, h_ref, dy_ref, g_ref, u_ref, wg_ref, wu_ref, wd_ref,
    dx_ref, ogu_ref, od_ref,
    a_s, dcur, da, p_s, dg_s, du_s, acc_g, acc_u, acc_d,
    st_gu, st_d, xs_gu, xs_d, xr_gu, xr_d, cs_gu, cs_d, cr_gu, cr_d, fo_gu, fo_d,
    in_sem, xs_sem, xr_sem, cs_sem, cr_sem, out_sem, xfree, cfree,
):
    p = pl.program_id(0)
    t = pl.program_id(1)
    rep = lax.axis_index("rep")
    me = lax.axis_index("dp")
    z, core = me // 2, me % 2
    partner = z * 2 + (1 - core)
    lo, hi = jnp.maximum(me - 2, 0), jnp.minimum(me + 2, DP - 1)

    @pl.when((p == 0) & (t == 0))
    def _():
        load = pltpu.make_async_copy(dy_ref, dcur, in_sem)
        load.start()
        barrier = pltpu.get_barrier_semaphore()
        pl.semaphore_signal(barrier, inc=1, device_id=(rep, partner), device_id_type=MESH)

        @pl.when(z > 0)
        def _():
            pl.semaphore_signal(barrier, inc=1, device_id=(rep, lo), device_id_type=MESH)

        @pl.when(z < 3)
        def _():
            pl.semaphore_signal(barrier, inc=1, device_id=(rep, hi), device_id_type=MESH)

        pl.semaphore_wait(barrier, jnp.where((z == 0) | (z == 3), 2, 3))
        load.wait()
        acc_g[...] = jnp.zeros_like(acc_g)
        acc_u[...] = jnp.zeros_like(acc_u)
        acc_d[...] = jnp.zeros_like(acc_d)

    def swap(b):
        return [
            pltpu.make_async_remote_copy(
                src_ref=s.at[b], dst_ref=r.at[b], send_sem=xs_sem.at[b, i], recv_sem=xr_sem.at[b, i],
                device_id=(rep, partner), device_id_type=MESH,
            )
            for i, (s, r) in enumerate(((xs_gu, xr_gu), (xs_d, xr_d)))
        ]

    def hop(b, way, s, to):
        return [
            pltpu.make_async_remote_copy(
                src_ref=o.at[b, way, s], dst_ref=r.at[b, way, s],
                send_sem=cs_sem.at[b, way, s, i], recv_sem=cr_sem.at[b, way, s, i],
                device_id=(rep, to), device_id_type=MESH,
            )
            for i, (o, r) in enumerate(((cs_gu, cr_gu), (cs_d, cr_d)))
        ]

    def out_copies(b, ph):
        lay, c = 1 - ph // NCH, ph % NCH
        return [
            pltpu.make_async_copy(fo_gu.at[b], ogu_ref.at[lay, c], out_sem.at[b, 0]),
            pltpu.make_async_copy(fo_d.at[b], od_ref.at[lay, c], out_sem.at[b, 1]),
        ]

    def give(r):
        b = r % 2

        @pl.when(r >= 2)
        def _():
            pl.semaphore_wait(xfree.at[b], 1)
            for cp in swap(b):
                cp.wait_send()

        for dz in range(4):
            j = dz * 2 + (1 - core)
            rows = pl.ds(pl.multiple_of(j * DR, 16), DR)
            xs_gu[b, dz, 0] = acc_g[rows, :].astype(BF16)
            xs_gu[b, dz, 1] = acc_u[rows, :].astype(BF16)
            xs_d[b, dz] = acc_d[pl.ds(pl.multiple_of(j * KR, 16), KR), :].astype(BF16)
        for cp in swap(b):
            cp.start()
        for dz in range(4):
            j = dz * 2 + core
            rows = pl.ds(pl.multiple_of(j * DR, 16), DR)
            st_gu[b, dz, 0] = acc_g[rows, :]
            st_gu[b, dz, 1] = acc_u[rows, :]
            st_d[b, dz] = acc_d[pl.ds(pl.multiple_of(j * KR, 16), KR), :]
        acc_g[...] = jnp.zeros_like(acc_g)
        acc_u[...] = jnp.zeros_like(acc_u)
        acc_d[...] = jnp.zeros_like(acc_d)

    def take(r):
        b = r % 2
        for cp in swap(b):
            cp.wait_recv()
        st_gu[b] += xr_gu[b].astype(F32)
        st_d[b] += xr_d[b].astype(F32)

        @pl.when(r < NP - 2)
        def _():
            pl.semaphore_signal(xfree.at[b], inc=1, device_id=(rep, partner), device_id_type=MESH)

    def send(r, s):
        b = r % 2
        for way in range(2):
            zz = z if way == 0 else 3 - z
            to = hi if way == 0 else lo

            @pl.when(zz <= s)
            def _(zz=zz, to=to, way=way):
                dest = 3 - s + zz
                dest = jnp.minimum(dest, 3)
                dest = dest if way == 0 else 3 - dest
                copies = hop(b, way, s, to)

                if s < 3:
                    @pl.when((r >= 2) & (zz == s))
                    def _():
                        pl.semaphore_wait(cfree.at[b, way], 1)

                    @pl.when(r >= 2)
                    def _():
                        for cp in copies:
                            cp.wait_send()

                @pl.when(zz == 0)
                def _():
                    cs_gu[b, way, s] = st_gu[b, dest].astype(BF16)
                    cs_d[b, way, s] = st_d[b, dest].astype(BF16)

                if s > 0:
                    @pl.when(zz > 0)
                    def _():
                        for cp in hop(b, way, s - 1, to):
                            cp.wait_recv()
                        cs_gu[b, way, s] = (st_gu[b, dest] + cr_gu[b, way, s - 1].astype(F32)).astype(BF16)
                        cs_d[b, way, s] = (st_d[b, dest] + cr_d[b, way, s - 1].astype(F32)).astype(BF16)

                for cp in copies:
                    cp.start()

    def finish(r):
        b = r % 2
        for way in range(2):
            zz = z if way == 0 else 3 - z
            to = hi if way == 0 else lo
            back = lo if way == 0 else hi

            @pl.when(zz > 0)
            def _(way=way, to=to, back=back):
                for cp in hop(b, way, 2, to):
                    cp.wait_recv()
                st_gu[b, z] += cr_gu[b, way, 2].astype(F32)
                st_d[b, z] += cr_d[b, way, 2].astype(F32)

                @pl.when(r < NP - 2)
                def _():
                    pl.semaphore_signal(cfree.at[b, way], inc=1, device_id=(rep, back), device_id_type=MESH)

        @pl.when(r >= 2)
        def _():
            for cp in out_copies(b, r - 2):
                cp.wait()

        fo_gu[b] = st_gu[b, z].astype(BF16)
        fo_d[b] = st_d[b, z].astype(BF16)
        for cp in out_copies(b, r):
            cp.start()

    @pl.when(p < NP)
    def compute():
        c = p % NCH
        tok = pl.multiple_of(t * T, T)

        def norm_into(src):
            for i in range(T // SUB):
                rows = pl.ds(i * SUB, SUB)
                h = src[rows, :].astype(F32)
                a_s[rows, :] = (h * scale_of(h)).astype(BF16)

        wg = wg_ref[...].reshape(D, CW)
        wu = wu_ref[...].reshape(D, CW)
        wd = wd_ref[...].reshape(CW, D)

        def elementwise(g, u, i):
            rows = pl.ds(i * SUB, SUB)
            dp = dot(dcur[pl.ds(tok + i * SUB, SUB), :], wd, 1, 1).astype(BF16).astype(F32)
            s = sigmoid(g)
            act = g * s
            p_s[rows, :] = (act * u).astype(BF16)
            du_s[rows, :] = (act * dp).astype(BF16)
            dg_s[rows, :] = (dp * u * (s + act * (1.0 - s))).astype(BF16)

        @pl.when(p < NCH)
        def _():
            norm_into(h_ref)
            for i in range(T // SUB):
                a = a_s[pl.ds(i * SUB, SUB), :]
                elementwise(dot(a, wg, 1, 0), dot(a, wu, 1, 0), i)

        @pl.when(p >= NCH)
        def _():
            norm_into(x_ref)
            for i in range(T // SUB):
                rows = pl.ds(i * SUB, SUB)
                elementwise(g_ref[rows, :], u_ref[rows, :], i)

        a = a_s[...]
        here = pl.ds(tok, T)
        acc_d[...] += dot(p_s[...], dcur[here, :], 0, 0)
        acc_g[...] += dot(a, dg_s[...], 0, 0)
        acc_u[...] += dot(a, du_s[...], 0, 0)

        @pl.when(c == 0)
        def _():
            da[here, :] = dot(dg_s[...], wg, 1, 1) + dot(du_s[...], wu, 1, 1)

        @pl.when(c > 0)
        def _():
            da[here, :] += dot(dg_s[...], wg, 1, 1) + dot(du_s[...], wu, 1, 1)

        def through_norm(src):
            for i in range(T // SUB):
                rows = pl.ds(i * SUB, SUB)
                glob = pl.ds(tok + i * SUB, SUB)
                h = src[rows, :].astype(F32)
                m = scale_of(h)
                d = da[glob, :].astype(BF16).astype(F32)
                k = jnp.sum(h * d, -1, keepdims=True) * (m * m * m) * (-1.0 / D)
                new = dcur[glob, :] + (d * m + h * k).astype(BF16)
                dcur[glob, :] = new
                dx_ref[rows, :] = new

        @pl.when(p == NCH - 1)
        def _():
            through_norm(h_ref)

        @pl.when(p == NP - 1)
        def _():
            through_norm(x_ref)

    one, two = (p >= 1) & (p - 1 < NP), (p >= 2) & (p - 2 < NP)

    @pl.when((t == 0) & two)
    def _():
        send(p - 2, 2)

    @pl.when((t == 0) & one)
    def _():
        take(p - 1)
        send(p - 1, 0)

    @pl.when((t == NT // 2) & two)
    def _():
        finish(p - 2)

    @pl.when((t == NT // 2) & one)
    def _():
        send(p - 1, 1)

    @pl.when((t == NT - 1) & (p < NP))
    def _():
        give(p)

    @pl.when((p == NP + 1) & (t == NT - 1))
    def _():
        for r in (NP - 2, NP - 1):
            b = r % 2
            for cp in swap(b):
                cp.wait_send()
            for way in range(2):
                zz = z if way == 0 else 3 - z
                for s in range(3):
                    @pl.when(zz <= s)
                    def _(way=way, s=s, b=b):
                        for cp in hop(b, way, s, hi if way == 0 else lo):
                            cp.wait_send()
            for cp in out_copies(b, r):
                cp.wait()


def backward(x, h, dy, g, u, wg, wu, wd):
    def phase(p):
        return jnp.minimum(p, NP - 1)

    def w_map(p, t):
        q = phase(p)
        return (0, 1 - q // NCH, q % NCH, 0, 0)

    late = lambda p, t: jnp.where(p >= NP, NT - 1, jnp.where(p >= NCH, t, 0))
    gu_spec = pl.BlockSpec((T, CW), lambda p, t: (late(p, t), jnp.where(p >= NCH, phase(p) % NCH, 0)))
    any_spec = pl.BlockSpec(memory_space=pl.ANY)
    vm = pltpu.VMEM
    return pl.pallas_call(
        backward_kernel,
        grid=(NP + 2, NT),
        in_specs=[
            pl.BlockSpec((T, D), lambda p, t: (late(p, t), 0)),
            pl.BlockSpec((T, D), lambda p, t: (jnp.where(p < NCH, t, NT - 1), 0)),
            any_spec,
            gu_spec,
            gu_spec,
            pl.BlockSpec((DP, None, None, DR, CW), w_map),
            pl.BlockSpec((DP, None, None, DR, CW), w_map),
            pl.BlockSpec((DP, None, None, KR, D), w_map),
        ],
        out_specs=[
            pl.BlockSpec((T, D), lambda p, t: (jnp.where(p >= NP, NT - 1, jnp.where(p == NP - 1, t, 0)), 0)),
            any_spec,
            any_spec,
        ],
        out_shape=[
            jax.ShapeDtypeStruct((TOK, D), BF16),
            jax.ShapeDtypeStruct((L, NCH, 2, DR, CW), BF16),
            jax.ShapeDtypeStruct((L, NCH, KR, D), BF16),
        ],
        scratch_shapes=[
            vm((T, D), BF16), vm((TOK, D), BF16), vm((TOK, D), F32),
            vm((T, CW), BF16), vm((T, CW), BF16), vm((T, CW), BF16),
            vm((D, CW), F32), vm((D, CW), F32), vm((CW, D), F32),
            vm((2, 4, 2, DR, CW), F32), vm((2, 4, KR, D), F32),
            vm((2, 4, 2, DR, CW), BF16), vm((2, 4, KR, D), BF16),
            vm((2, 4, 2, DR, CW), BF16), vm((2, 4, KR, D), BF16),
            vm((2, 2, 3, 2, DR, CW), BF16), vm((2, 2, 3, KR, D), BF16),
            vm((2, 2, 3, 2, DR, CW), BF16), vm((2, 2, 3, KR, D), BF16),
            vm((2, 2, DR, CW), BF16), vm((2, KR, D), BF16),
            pltpu.SemaphoreType.DMA,
            pltpu.SemaphoreType.DMA((2, 2)), pltpu.SemaphoreType.DMA((2, 2)),
            pltpu.SemaphoreType.DMA((2, 2, 3, 2)), pltpu.SemaphoreType.DMA((2, 2, 3, 2)),
            pltpu.SemaphoreType.DMA((2, 2)),
            pltpu.SemaphoreType.REGULAR((2,)), pltpu.SemaphoreType.REGULAR((2, 2)),
        ],
        compiler_params=pltpu.CompilerParams(
            vmem_limit_bytes=VMEM_LIMIT, collective_id=1, has_side_effects=True,
            dimension_semantics=("arbitrary", "arbitrary"),
        ),
        cost_estimate=pl.CostEstimate(flops=28 * TOK * D * FF, bytes_accessed=10**8, transcendentals=0),
        name="backward",
    )(x, h, dy, g, u, wg, wu, wd)


def solution(mesh):
    def body(x, dy, w_gate, w_up, w_down):
        x, dy = x[0], dy[0]
        split = lambda w: w.reshape(L, DR, DP, NCH, KR).transpose(0, 3, 1, 2, 4).reshape(L, NCH, DR, CW)
        gather = lambda w: lax.all_gather(w, "dp", axis=0, tiled=False)
        wg, wu = gather(split(w_gate)), gather(split(w_up))
        wd = gather(w_down.reshape(L, NCH, KR, D))
        g, u, h = forward(x, wg, wu, wd)
        dx, ogu, od = backward(x, h, dy, g, u, wg, wu, wd)
        join = lambda o: o.reshape(L, NCH, DR, DP, KR).transpose(0, 2, 3, 1, 4).reshape(L, DR, FF)
        return dx[None], join(ogu[:, :, 0]), join(ogu[:, :, 1]), od.reshape(L, NCH * KR, D)

    rows = P(None, "dp", None)
    seqs = P(("rep", "dp"), None, None)
    outs = P("rep", "dp", None)
    return jax.shard_map(
        body, mesh=mesh, in_specs=(seqs, seqs, rows, rows, rows), out_specs=(seqs, outs, outs, outs), check_vma=False
    )
```

```python
import functools

import jax
import jax.numpy as jnp
from jax import lax
from jax.experimental import pallas as pl
from jax.experimental.pallas import tpu as pltpu
from jax.sharding import PartitionSpec as P

TOK, D, FF, L, DP = 4096, 896, 2304, 2, 8
CW = 256
NCH = FF // CW
KR = FF // DP // NCH
DR = D // DP
T = 1024
NT = TOK // T
SUB = 256
FSUB = 256
TB = 512
NP = L * NCH
EPS = 1e-6
MESH = pl.DeviceIdType.MESH
F32, BF16 = jnp.float32, jnp.bfloat16
VMEM_LIMIT = 67_043_328


def dot(a, b, ca, cb):
    return lax.dot_general(a, b, (((ca,), (cb,)), ((), ())), preferred_element_type=F32)


def sigmoid(g):
    return 0.5 * jnp.tanh(0.5 * g) + 0.5


def scale_of(h):
    return lax.rsqrt(jnp.mean(h * h, -1, keepdims=True) + EPS)


def gate_up_kernel(keep_p, x_ref, wg_ref, wu_ref, *refs):
    g_ref, u_ref, a_ref = refs[:3] if keep_p else refs[3:6]

    @pl.when(pl.program_id(1) == 0)
    def _():
        for i in range(T // SUB):
            rows = pl.ds(i * SUB, SUB)
            h = x_ref[rows, :].astype(F32)
            a_ref[rows, :] = (h * scale_of(h)).astype(BF16)

    wg = wg_ref[...].reshape(D, CW)
    wu = wu_ref[...].reshape(D, CW)
    for i in range(T // FSUB):
        rows = pl.ds(i * FSUB, FSUB)
        a = a_ref[rows, :]
        g = dot(a, wg, 1, 0)
        u = dot(a, wu, 1, 0)
        g_ref[rows, :] = g
        u_ref[rows, :] = u
        if keep_p:
            refs[3][rows, :] = (g * sigmoid(g) * u).astype(BF16)


def gate_up(layer, x, wgu, *before):
    keep_p = layer == 0
    tile = pl.BlockSpec((None, T, CW), lambda t, c: (layer, t, c))
    wide = jax.ShapeDtypeStruct((L, TOK, FF), F32)
    p_spec, p_shape = [pl.BlockSpec((T, CW), lambda t, c: (t, c))], [jax.ShapeDtypeStruct((TOK, FF), BF16)]
    return pl.pallas_call(
        functools.partial(gate_up_kernel, keep_p),
        grid=(NT, NCH),
        in_specs=[
            pl.BlockSpec((T, D), lambda t, c: (t, 0)),
            pl.BlockSpec((DP, None, DR, CW), lambda t, c: (0, c, 0, 0)),
            pl.BlockSpec((DP, None, DR, CW), lambda t, c: (0, NCH + c, 0, 0)),
        ] + [pl.BlockSpec(memory_space=pl.ANY)] * len(before),
        out_specs=[tile, tile, pl.BlockSpec((None, T, D), lambda t, c: (layer, t, 0))] + p_spec * keep_p,
        out_shape=[wide, wide, jax.ShapeDtypeStruct((L, TOK, D), BF16)] + p_shape * keep_p,
        input_output_aliases={3 + i: i for i in range(len(before))},
        compiler_params=pltpu.CompilerParams(
            vmem_limit_bytes=VMEM_LIMIT, dimension_semantics=("arbitrary", "arbitrary")
        ),
        cost_estimate=pl.CostEstimate(flops=4 * TOK * D * FF, bytes_accessed=10**8, transcendentals=0),
        name=f"gate_up_{layer}",
    )(x, wgu, wgu, *before)


def down_kernel(x_ref, p_ref, wd_ref, h_ref, w_s):
    @pl.when(pl.program_id(0) == 0)
    def _():
        for c in range(NCH):
            w_s[pl.ds(c * CW, CW), :] = wd_ref[:, c].reshape(CW, D)

    for i in range(TB // SUB):
        rows = pl.ds(i * SUB, SUB)
        h_ref[rows, :] = x_ref[rows, :] + dot(p_ref[rows, :], w_s[...], 1, 0).astype(BF16)


def down(x, p, wd):
    return pl.pallas_call(
        down_kernel,
        grid=(TOK // TB,),
        in_specs=[
            pl.BlockSpec((TB, D), lambda t: (t, 0)),
            pl.BlockSpec((TB, FF), lambda t: (t, 0)),
            pl.BlockSpec((DP, NCH, KR, D), lambda t: (0, 0, 0, 0)),
        ],
        out_specs=pl.BlockSpec((TB, D), lambda t: (t, 0)),
        out_shape=jax.ShapeDtypeStruct((TOK, D), BF16),
        scratch_shapes=[pltpu.VMEM((FF, D), BF16)],
        compiler_params=pltpu.CompilerParams(vmem_limit_bytes=VMEM_LIMIT, dimension_semantics=("arbitrary",)),
        cost_estimate=pl.CostEstimate(flops=2 * TOK * D * FF, bytes_accessed=4 * 10**7, transcendentals=0),
        name="down",
    )(x, p, wd)


def backward_kernel(
    x_ref, h_ref, a_ref, dy_ref, g_ref, u_ref, wg2_ref, wu2_ref, wd2_ref, wg1_ref, wu1_ref, wd1_ref,
    dx_ref, ogu_ref, od_ref,
    wg_s, wu_s, wd_s, dcur, da, p_s, dg_s, du_s, acc_g, acc_u, acc_d,
    st_gu, st_d, xs_gu, xs_d, xr_gu, xr_d, cs_gu, cs_d, cr_gu, cr_d, fo_gu, fo_d,
    in_sem, xs_sem, xr_sem, cs_sem, cr_sem, out_sem, xfree, cfree,
):
    p = pl.program_id(0)
    t = pl.program_id(1)
    rep = lax.axis_index("rep")
    me = lax.axis_index("dp")
    z, core = me // 2, me % 2
    partner = z * 2 + (1 - core)
    lo, hi = jnp.maximum(me - 2, 0), jnp.minimum(me + 2, DP - 1)

    @pl.when((p == 0) & (t == 0))
    def _():
        load = pltpu.make_async_copy(dy_ref, dcur, in_sem)
        load.start()
        barrier = pltpu.get_barrier_semaphore()
        pl.semaphore_signal(barrier, inc=1, device_id=(rep, partner), device_id_type=MESH)

        @pl.when(z > 0)
        def _():
            pl.semaphore_signal(barrier, inc=1, device_id=(rep, lo), device_id_type=MESH)

        @pl.when(z < 3)
        def _():
            pl.semaphore_signal(barrier, inc=1, device_id=(rep, hi), device_id_type=MESH)

        pl.semaphore_wait(barrier, jnp.where((z == 0) | (z == 3), 2, 3))
        load.wait()
        acc_g[...] = jnp.zeros_like(acc_g)
        acc_u[...] = jnp.zeros_like(acc_u)
        acc_d[...] = jnp.zeros_like(acc_d)

    def swap(b):
        return [
            pltpu.make_async_remote_copy(
                src_ref=s.at[b], dst_ref=r.at[b], send_sem=xs_sem.at[b, i], recv_sem=xr_sem.at[b, i],
                device_id=(rep, partner), device_id_type=MESH,
            )
            for i, (s, r) in enumerate(((xs_gu, xr_gu), (xs_d, xr_d)))
        ]

    def hop(b, way, s, to):
        return [
            pltpu.make_async_remote_copy(
                src_ref=o.at[b, way, s], dst_ref=r.at[b, way, s],
                send_sem=cs_sem.at[b, way, s, i], recv_sem=cr_sem.at[b, way, s, i],
                device_id=(rep, to), device_id_type=MESH,
            )
            for i, (o, r) in enumerate(((cs_gu, cr_gu), (cs_d, cr_d)))
        ]

    def out_copies(b, ph):
        lay, c = 1 - ph // NCH, ph % NCH
        return [
            pltpu.make_async_copy(fo_gu.at[b], ogu_ref.at[lay, c], out_sem.at[b, 0]),
            pltpu.make_async_copy(fo_d.at[b], od_ref.at[lay, c], out_sem.at[b, 1]),
        ]

    def give(r):
        b = r % 2

        @pl.when(r >= 2)
        def _():
            pl.semaphore_wait(xfree.at[b], 1)
            for cp in swap(b):
                cp.wait_send()

        for dz in range(4):
            j = dz * 2 + (1 - core)
            rows = pl.ds(pl.multiple_of(j * DR, 16), DR)
            xs_gu[b, dz, 0] = acc_g[rows, :].astype(BF16)
            xs_gu[b, dz, 1] = acc_u[rows, :].astype(BF16)
            xs_d[b, dz] = acc_d[pl.ds(pl.multiple_of(j * KR, 16), KR), :].astype(BF16)
        for cp in swap(b):
            cp.start()
        for dz in range(4):
            j = dz * 2 + core
            rows = pl.ds(pl.multiple_of(j * DR, 16), DR)
            st_gu[b, dz, 0] = acc_g[rows, :]
            st_gu[b, dz, 1] = acc_u[rows, :]
            st_d[b, dz] = acc_d[pl.ds(pl.multiple_of(j * KR, 16), KR), :]
        acc_g[...] = jnp.zeros_like(acc_g)
        acc_u[...] = jnp.zeros_like(acc_u)
        acc_d[...] = jnp.zeros_like(acc_d)

    def take(r):
        b = r % 2
        for cp in swap(b):
            cp.wait_recv()
        st_gu[b] += xr_gu[b].astype(F32)
        st_d[b] += xr_d[b].astype(F32)

        @pl.when(r < NP - 2)
        def _():
            pl.semaphore_signal(xfree.at[b], inc=1, device_id=(rep, partner), device_id_type=MESH)

    def send(r, s):
        b = r % 2
        for way in range(2):
            zz = z if way == 0 else 3 - z
            to = hi if way == 0 else lo

            @pl.when(zz <= s)
            def _(zz=zz, to=to, way=way):
                dest = 3 - s + zz
                dest = jnp.minimum(dest, 3)
                dest = dest if way == 0 else 3 - dest
                copies = hop(b, way, s, to)

                if s < 3:
                    @pl.when((r >= 2) & (zz == s))
                    def _():
                        pl.semaphore_wait(cfree.at[b, way], 1)

                    @pl.when(r >= 2)
                    def _():
                        for cp in copies:
                            cp.wait_send()

                @pl.when(zz == 0)
                def _():
                    cs_gu[b, way, s] = st_gu[b, dest].astype(BF16)
                    cs_d[b, way, s] = st_d[b, dest].astype(BF16)

                if s > 0:
                    @pl.when(zz > 0)
                    def _():
                        for cp in hop(b, way, s - 1, to):
                            cp.wait_recv()
                        cs_gu[b, way, s] = (st_gu[b, dest] + cr_gu[b, way, s - 1].astype(F32)).astype(BF16)
                        cs_d[b, way, s] = (st_d[b, dest] + cr_d[b, way, s - 1].astype(F32)).astype(BF16)

                for cp in copies:
                    cp.start()

    def finish(r):
        b = r % 2
        for way in range(2):
            zz = z if way == 0 else 3 - z
            to = hi if way == 0 else lo
            back = lo if way == 0 else hi

            @pl.when(zz > 0)
            def _(way=way, to=to, back=back):
                for cp in hop(b, way, 2, to):
                    cp.wait_recv()
                st_gu[b, z] += cr_gu[b, way, 2].astype(F32)
                st_d[b, z] += cr_d[b, way, 2].astype(F32)

                @pl.when(r < NP - 2)
                def _():
                    pl.semaphore_signal(cfree.at[b, way], inc=1, device_id=(rep, back), device_id_type=MESH)

        @pl.when(r >= 2)
        def _():
            for cp in out_copies(b, r - 2):
                cp.wait()

        fo_gu[b] = st_gu[b, z].astype(BF16)
        fo_d[b] = st_d[b, z].astype(BF16)
        for cp in out_copies(b, r):
            cp.start()

    @pl.when(p < NP)
    def compute():
        c = p % NCH
        tok = pl.multiple_of(t * T, T)

        for mine, of_layer in ((p < NCH, (wg2_ref, wu2_ref, wd2_ref)), (p >= NCH, (wg1_ref, wu1_ref, wd1_ref))):
            @pl.when(mine & (t == 0))
            def _(of_layer=of_layer):
                wg_s[...] = of_layer[0][...].reshape(D, CW)
                wu_s[...] = of_layer[1][...].reshape(D, CW)
                wd_s[...] = of_layer[2][...].reshape(CW, D)

        for i in range(T // SUB):
            rows = pl.ds(i * SUB, SUB)
            g, u = g_ref[rows, :], u_ref[rows, :]
            dp = dot(dcur[pl.ds(tok + i * SUB, SUB), :], wd_s[...], 1, 1).astype(BF16).astype(F32)
            s = sigmoid(g)
            act = g * s
            p_s[rows, :] = (act * u).astype(BF16)
            du_s[rows, :] = (act * dp).astype(BF16)
            dg_s[rows, :] = (dp * u * (s + act * (1.0 - s))).astype(BF16)

        a, wg, wu = a_ref[...], wg_s[...], wu_s[...]
        here = pl.ds(tok, T)
        acc_d[...] += dot(p_s[...], dcur[here, :], 0, 0)
        acc_g[...] += dot(a, dg_s[...], 0, 0)
        acc_u[...] += dot(a, du_s[...], 0, 0)

        @pl.when(c == 0)
        def _():
            da[here, :] = dot(dg_s[...], wg, 1, 1) + dot(du_s[...], wu, 1, 1)

        @pl.when(c > 0)
        def _():
            da[here, :] += dot(dg_s[...], wg, 1, 1) + dot(du_s[...], wu, 1, 1)

        def through_norm(src):
            for i in range(T // SUB):
                rows = pl.ds(i * SUB, SUB)
                glob = pl.ds(tok + i * SUB, SUB)
                h = src[rows, :].astype(F32)
                m = scale_of(h)
                d = da[glob, :].astype(BF16).astype(F32)
                k = jnp.sum(h * d, -1, keepdims=True) * (m * m * m) * (-1.0 / D)
                new = dcur[glob, :] + (d * m + h * k).astype(BF16)
                dcur[glob, :] = new
                dx_ref[rows, :] = new

        @pl.when(p == NCH - 1)
        def _():
            through_norm(h_ref)

        @pl.when(p == NP - 1)
        def _():
            through_norm(x_ref)

    one, two = (p >= 1) & (p - 1 < NP), (p >= 2) & (p - 2 < NP)

    @pl.when((t == 0) & two)
    def _():
        send(p - 2, 2)

    @pl.when((t == 0) & one)
    def _():
        take(p - 1)
        send(p - 1, 0)

    @pl.when((t == NT // 2) & two)
    def _():
        finish(p - 2)

    @pl.when((t == NT // 2) & one)
    def _():
        send(p - 1, 1)

    @pl.when((t == NT - 1) & (p < NP))
    def _():
        give(p)

    @pl.when((p == NP + 1) & (t == NT - 1))
    def _():
        for r in (NP - 2, NP - 1):
            b = r % 2
            for cp in swap(b):
                cp.wait_send()
            for way in range(2):
                zz = z if way == 0 else 3 - z
                for s in range(3):
                    @pl.when(zz <= s)
                    def _(way=way, s=s, b=b):
                        for cp in hop(b, way, s, hi if way == 0 else lo):
                            cp.wait_send()
            for cp in out_copies(b, r):
                cp.wait()


def backward(x, h, a, dy, g, u, wgu1, wd1, wgu2, wd2):
    def phase(p):
        return jnp.minimum(p, NP - 1)

    def chunk(lay, p):
        return jnp.minimum(p, NCH - 1) if lay else jnp.maximum(phase(p) - NCH, 0)

    def w_specs(lay):
        return [
            pl.BlockSpec((DP, None, DR, CW), lambda p, t: (0, chunk(lay, p), 0, 0)),
            pl.BlockSpec((DP, None, DR, CW), lambda p, t: (0, NCH + chunk(lay, p), 0, 0)),
            pl.BlockSpec((DP, None, KR, D), lambda p, t: (0, chunk(lay, p), 0, 0)),
        ]

    layer = lambda p: 1 - phase(p) // NCH
    row = lambda p, t: jnp.where(p >= NP, NT - 1, t)
    gu_spec = pl.BlockSpec((None, T, CW), lambda p, t: (layer(p), row(p, t), phase(p) % NCH))
    any_spec = pl.BlockSpec(memory_space=pl.ANY)
    vm = pltpu.VMEM
    return pl.pallas_call(
        backward_kernel,
        grid=(NP + 2, NT),
        in_specs=[
            pl.BlockSpec(
                (T, D), lambda p, t: (jnp.where(p >= NP, NT - 1, jnp.where(p == NP - 1, t, 0)), 0),
                pipeline_mode=pl.Buffered(1),
            ),
            pl.BlockSpec(
                (T, D), lambda p, t: (jnp.where(p >= NCH, NT - 1, jnp.where(p == NCH - 1, t, 0)), 0),
                pipeline_mode=pl.Buffered(1),
            ),
            pl.BlockSpec((None, T, D), lambda p, t: (layer(p), row(p, t), 0)),
            any_spec,
            gu_spec,
            gu_spec,
            *w_specs(1),
            *w_specs(0),
        ],
        out_specs=[
            pl.BlockSpec((T, D), lambda p, t: (jnp.where(p >= NP, NT - 1, jnp.where(p == NP - 1, t, 0)), 0)),
            any_spec,
            any_spec,
        ],
        out_shape=[
            jax.ShapeDtypeStruct((TOK, D), BF16),
            jax.ShapeDtypeStruct((L, NCH, 2, DR, CW), BF16),
            jax.ShapeDtypeStruct((L, NCH, KR, D), BF16),
        ],
        scratch_shapes=[
            vm((D, CW), BF16), vm((D, CW), BF16), vm((CW, D), BF16), vm((TOK, D), BF16), vm((TOK, D), F32),
            vm((T, CW), BF16), vm((T, CW), BF16), vm((T, CW), BF16),
            vm((D, CW), F32), vm((D, CW), F32), vm((CW, D), F32),
            vm((2, 4, 2, DR, CW), F32), vm((2, 4, KR, D), F32),
            vm((2, 4, 2, DR, CW), BF16), vm((2, 4, KR, D), BF16),
            vm((2, 4, 2, DR, CW), BF16), vm((2, 4, KR, D), BF16),
            vm((2, 2, 3, 2, DR, CW), BF16), vm((2, 2, 3, KR, D), BF16),
            vm((2, 2, 3, 2, DR, CW), BF16), vm((2, 2, 3, KR, D), BF16),
            vm((2, 2, DR, CW), BF16), vm((2, KR, D), BF16),
            pltpu.SemaphoreType.DMA,
            pltpu.SemaphoreType.DMA((2, 2)), pltpu.SemaphoreType.DMA((2, 2)),
            pltpu.SemaphoreType.DMA((2, 2, 3, 2)), pltpu.SemaphoreType.DMA((2, 2, 3, 2)),
            pltpu.SemaphoreType.DMA((2, 2)),
            pltpu.SemaphoreType.REGULAR((2,)), pltpu.SemaphoreType.REGULAR((2, 2)),
        ],
        compiler_params=pltpu.CompilerParams(
            vmem_limit_bytes=VMEM_LIMIT, collective_id=1, has_side_effects=True,
            dimension_semantics=("arbitrary", "arbitrary"),
        ),
        cost_estimate=pl.CostEstimate(flops=28 * TOK * D * FF, bytes_accessed=10**8, transcendentals=0),
        name="backward",
    )(x, h, a, dy, g, u, wgu2, wgu2, wd2, wgu1, wgu1, wd1)


def solution(mesh):
    def body(x, dy, w_gate, w_up, w_down):
        x, dy = x[0], dy[0]
        split = lambda w: w.reshape(DR, DP, NCH, KR).transpose(2, 0, 1, 3).reshape(NCH, DR, CW)
        gather = lambda w: lax.all_gather(w, "dp", axis=0, tiled=False)
        w_down = w_down.reshape(L, NCH, KR, D)
        wgu1 = gather(jnp.concatenate([split(w_gate[0]), split(w_up[0])]))
        wd1 = gather(w_down[0])
        wgu2 = gather(jnp.concatenate([split(w_gate[1]), split(w_up[1])]))
        wd2 = gather(w_down[1])
        g, u, a, p = gate_up(0, x, wgu1)
        h = down(x, p, wd1)
        g, u, a = gate_up(1, h, wgu2, g, u, a)
        dx, ogu, od = backward(x, h, a, dy, g, u, wgu1, wd1, wgu2, wd2)
        join = lambda o: o.reshape(L, NCH, DR, DP, KR).transpose(0, 2, 3, 1, 4).reshape(L, DR, FF)
        return dx[None], join(ogu[:, :, 0]), join(ogu[:, :, 1]), od.reshape(L, NCH * KR, D)

    rows = P(None, "dp", None)
    seqs = P(("rep", "dp"), None, None)
    outs = P("rep", "dp", None)
    return jax.shard_map(
        body, mesh=mesh, in_specs=(seqs, seqs, rows, rows, rows), out_specs=(seqs, outs, outs, outs), check_vma=False
    )
```
